32 devices in a mesh: dom: 32 (over z, y, x, core).
Axes of the slice: x: 2, y: 2, z: 4, core: 2. Of those that a mesh axis runs over, the one named last changes fastest.
Arguments:
- wing_jitter: float32 [3, 262144], P(None, 'dom'), may hold values from 0 to 1
- live_blocks: int32 [32], P('dom'), may hold values from 1 to 64, as said below
- smoothing: float32 [262144], P('dom'), may hold values from 0.3 to 3
- displacement: float32 [3, 262144], P(None, 'dom'), may hold values from -20 to 20
- fluid_jitter: float32 [3, 98304], P(None, 'dom'), may hold values from 0 to 1
Outputs:
- coefs: float32 [3, 262144], P(None, 'dom')
- residual: float32 [3, 262144], P(None, 'dom')
- fluid_values: float32 [3, 98304], P(None, 'dom')
The draws below stay inside these ranges and needn't reach their ends.
Inputs may be any that keep to these rules, and one draw needn't show every extreme that they name: `live_blocks`: some device holds 64 live blocks, and some device other than the first and the last holds 1.
All inputs are finite; a program needn't handle non-finite values.
Results may differ from the reference program's by a relative error of at most 0.0003.
Values sent between devices are 32-bit elements; how exact they have to be, the bound alone decides.
A program may use at most 64 MiB of HBM per device.

```python
import math
import jax
import jax.numpy as jnp
from jax import lax

BLK = 128
NBD = 64
FB = 24
ITERS = 3
ROWS = 262144
FROWS = 98304
N_DOM = 32


def draw_live_blocks(key, part):
    key_counts, key_small, key_large = jax.random.split(key, 3)
    counts = jax.random.randint(key_counts, (N_DOM,), 1, NBD + 1)
    small_index = jax.random.randint(key_small, (), 1, N_DOM - 1)
    large_index = (small_index + 1 + jax.random.randint(key_large, (), 0, N_DOM - 2)) % N_DOM
    places = jnp.arange(N_DOM)
    counts = jnp.where(places == large_index, NBD, counts)
    counts = jnp.where(places == small_index, 1, counts)
    return counts.astype(jnp.int32)


def draw_displacement(key, part):
    key_values = jax.random.fold_in(key, 0)
    values = jax.random.truncated_normal(key_values, -6.0, 6.0, (3, ROWS), jnp.float32)
    rising = 1.0 + 2.0 * jnp.arange(ROWS, dtype=jnp.float32) / (ROWS - 1)
    values = values * rising[None, :]
    return values


def shard_levels(key, extent, shards, smallest, largest):
    level = 1.0
    for position, shards_of in shards:
        steps = jax.random.uniform(jax.random.fold_in(jax.random.fold_in(key, 6), position), (shards_of,), jnp.float32, smallest / len(shards), largest / len(shards))
        level = level * jnp.repeat(jnp.exp(steps), extent[position] // shards_of).reshape((-1,) + (1,) * (len(extent) - 1 - position))
    return level


def setup_inputs(seed: int = 0) -> dict:
    splits = jax.random.split(jax.random.key(seed), 6)
    return {
        "wing_jitter": jnp.clip(1.0 * jax.random.uniform(splits[0], (3, ROWS), jnp.float32) ** shard_levels(splits[0], (3, ROWS), ((1, 32),), -0.2, 0.2), 0.0, 1.0),
        "live_blocks": draw_live_blocks(jax.random.fold_in(splits[5], 71), 0),
        "smoothing": jnp.clip(jnp.exp(math.log(3.0) - 2.3025851 * jax.random.uniform(splits[2], (ROWS,), jnp.float32) ** shard_levels(splits[2], (ROWS,), ((0, 32),), -0.2, 0.2)), 0.3, 3.0),
        "displacement": draw_displacement(jax.random.fold_in(splits[5], 71), 0),
        "fluid_jitter": jnp.clip(1.0 * jax.random.uniform(splits[4], (3, FROWS), jnp.float32) ** shard_levels(splits[4], (3, FROWS), ((1, 32),), -0.2, 0.2), 0.0, 1.0),
    }


def wendland(row_points, col_points):
    spread = (row_points[0][:, None] - col_points[0][None, :]) ** 2
    spread = spread + (row_points[1][:, None] - col_points[1][None, :]) ** 2
    spread = spread + (row_points[2][:, None] - col_points[2][None, :]) ** 2
    scaled = jnp.sqrt(spread) * 0.5
    remain = jnp.maximum(1.0 - scaled, 0.0)
    return remain * remain * remain * remain * (4.0 * scaled + 1.0)

def reference(wing_jitter, live_blocks, smoothing, displacement, fluid_jitter):
    block_count = N_DOM * NBD
    starts = (jnp.cumsum(live_blocks) - live_blocks).astype(jnp.int32)
    total = jnp.sum(live_blocks).astype(jnp.int32)
    block_ids = jnp.arange(block_count, dtype=jnp.int32)
    owners = block_ids // NBD
    local_ids = block_ids % NBD
    valid = local_ids < live_blocks[owners]
    chain = (starts[owners] + local_ids).astype(jnp.int32)
    slots = jnp.where(valid, chain, block_count).astype(jnp.int32)
    lookup = jnp.zeros((block_count,), jnp.int32).at[slots].set(block_ids, mode='drop')
    scales = jnp.array([1.0, 6.0, 6.0], jnp.float32)[None, :, None]
    unit_x = jnp.array([1.0, 0.0, 0.0], jnp.float32)[:, None]
    wing = wing_jitter.reshape(3, block_count, BLK).transpose(1, 0, 2) * scales
    row_mask = jnp.repeat(valid.astype(jnp.float32), BLK)

    def band_sum(points, chain_at, usable, vectors):
        summed = jnp.zeros((3, BLK), jnp.float32)
        for delta in range(-2, 3):
            target = chain_at + delta
            usable_here = usable & (target >= 0) & (target < total)
            source = lookup[jnp.clip(target, 0, block_count - 1)]
            col_points = wing[source] + delta * unit_x
            kernel = wendland(points, col_points)
            product = jnp.dot(vectors[source], kernel.T, precision=lax.Precision.HIGHEST)
            summed = summed + jnp.where(usable_here, product, 0.0)
        return summed

    def apply(vector):
        blocks = vector.reshape(3, block_count, BLK).transpose(1, 0, 2)

        def one_block(index):
            return band_sum(wing[index], chain[index], valid[index], blocks)

        def one_group(indices):
            return jax.vmap(one_block)(indices)
        result = lax.map(one_group, block_ids.reshape(-1, 16))
        result = result.reshape(block_count, 3, BLK).transpose(1, 0, 2).reshape(3, -1)
        return result * row_mask + smoothing * vector
    rhs = displacement * row_mask
    diagonal = 1.0 + smoothing
    coefs = jnp.zeros_like(rhs)
    residual = rhs
    precond = residual / diagonal
    direction = precond
    norm_now = lax.optimization_barrier(jnp.sum(residual * precond, axis=1))
    for iteration in range(ITERS):
        image = apply(direction)
        step_size = norm_now / lax.optimization_barrier(jnp.sum(direction * image, axis=1))
        coefs = coefs + step_size[:, None] * direction
        residual = residual - step_size[:, None] * image
        precond = residual / diagonal
        norm_next = lax.optimization_barrier(jnp.sum(residual * precond, axis=1))
        direction = precond + (norm_next / norm_now)[:, None] * direction
        norm_now = norm_next
    fluid_count = N_DOM * FB
    fluid_ids = jnp.arange(fluid_count, dtype=jnp.int32)
    fluid_owner = fluid_ids // FB
    anchors = fluid_ids % FB * live_blocks[fluid_owner] // FB
    fluid_chain = (starts[fluid_owner] + anchors).astype(jnp.int32)
    fluid = fluid_jitter.reshape(3, fluid_count, BLK).transpose(1, 0, 2) * scales
    coef_blocks = coefs.reshape(3, block_count, BLK).transpose(1, 0, 2)

    def one_fluid(index):
        return band_sum(fluid[index], fluid_chain[index], jnp.array(True), coef_blocks)

    def fluid_group(indices):
        return jax.vmap(one_fluid)(indices)
    fluid_values = lax.map(fluid_group, fluid_ids.reshape(-1, 8))
    fluid_values = fluid_values.reshape(fluid_count, 3, BLK).transpose(1, 0, 2).reshape(3, -1)
    return (coefs, residual, fluid_values)
```

```python
import functools

import jax
import jax.numpy as jnp
from jax import lax
from jax.experimental import pallas as pl
from jax.experimental.pallas import tpu as pltpu
from jax.sharding import PartitionSpec as P

BLK = 128
ITERS = 3
BAND = 5
FAR = 1.0e4
F32 = jnp.float32
BF16 = jnp.bfloat16


def phi_of(row, col):
    dx = row[0] - col[0]
    dy = row[1] - col[1]
    dz = row[2] - col[2]
    spread = jnp.maximum(dx * dx + dy * dy + dz * dz, 1e-30)
    scaled = spread * lax.rsqrt(spread)
    remain = jnp.maximum(1.0 - scaled, 0.0)
    square = remain * remain
    return square * square * (5.0 - 4.0 * remain)


def build(dest, columns, first_col, row):
    for delta in range(BAND):
        at = pl.multiple_of(first_col + delta * BLK, BLK)
        cols = columns[pl.ds(at, BLK), :]
        value = phi_of([cols[:, c:c + 1] for c in range(3)], row)
        high = value.astype(BF16)
        low = (value - high.astype(F32)).astype(BF16)
        dest[delta * BLK:(delta + 1) * BLK, 0:BLK] = high
        dest[delta * BLK:(delta + 1) * BLK, BLK:] = low


def split(v):
    high = v.astype(BF16).astype(F32)
    return jnp.concatenate([high, v - high], axis=0).astype(BF16)


def solver(n_dev, nb, live_ref, wing_ref, smooth_ref, disp_ref,
           coef_out, resid_out, points, coef_ext,
           kmat, columns, ends, halo, sums, vext, zbuf, rbuf, dbuf, abuf, cbuf, ibuf, wbuf,
           inv, halo_send, halo_recv, sum_send, sum_recv):
    me = lax.axis_index("dom")
    count = live_ref[0]
    width = nb * BLK
    halo[...] = jnp.zeros_like(halo)
    barrier = pltpu.get_barrier_semaphore()

    def greet(k, carry):
        pl.semaphore_signal(barrier, inc=1, device_id=(lax.rem(me + k, n_dev),),
                            device_id_type=pl.DeviceIdType.MESH)
        return carry

    lax.fori_loop(1, n_dev, greet, 0)

    block_of = lax.broadcasted_iota(jnp.int32, (8, width), 1) >> 7
    live = block_of < count
    along_x = block_of.astype(F32)
    row_id = lax.broadcasted_iota(jnp.int32, (8, width), 0)
    zbuf[...] = jnp.zeros_like(zbuf)
    zbuf[0:3, :] = wing_ref[...]
    scale = jnp.where(row_id == 0, 0.5, 3.0)
    pts = zbuf[...] * scale + jnp.where(row_id == 0, along_x * 0.5, 0.0)
    pts = jnp.where(live, pts, FAR)
    points[:, 2 * BLK:2 * BLK + width] = pts
    smooth = jnp.broadcast_to(smooth_ref[...], (8, width))
    inv[...] = 1.0 / (1.0 + smooth)
    rbuf[...] = jnp.zeros_like(rbuf)
    rbuf[0:3, :] = disp_ref[...]
    rbuf[...] = jnp.where(live, rbuf[...], 0.0)
    zbuf[...] = rbuf[...] * inv[...]

    row8 = lax.broadcasted_iota(jnp.int32, (8, BLK), 0)
    lane8 = lax.broadcasted_iota(jnp.int32, (8, BLK), 1)

    def picked(ref, start, which):
        total = jnp.zeros((8, BLK), F32)
        for b in range(nb):
            total = total + jnp.where(which == b, ref[:, start + b * BLK:start + (b + 1) * BLK], 0.0)
        return total

    two = (count >= 2).astype(F32)

    def shifted(p, base):
        return jnp.where(row8 == 0, p - base * 0.5, p)

    def pack(p, z, flag):
        low = jnp.concatenate([p[0:3, :], z[0:3, :], jnp.full((2, BLK), 1.0, F32) * flag], axis=0)
        return low

    countf = count.astype(F32)
    own = 2 * BLK
    ends[0, 0, :, 0:BLK] = pack(shifted(picked(points, own, count - 2), countf), picked(zbuf, 0, count - 2), two)
    ends[0, 0, :, BLK:] = pack(shifted(picked(points, own, count - 1), countf), picked(zbuf, 0, count - 1), 1.0)
    ends[0, 1, :, 0:BLK] = pack(points[:, own:own + BLK], zbuf[:, 0:BLK], 1.0)
    ends[0, 1, :, BLK:] = pack(points[:, own + BLK:own + 2 * BLK], zbuf[:, BLK:2 * BLK], two)
    pl.semaphore_wait(barrier, n_dev - 1)

    def halo_copy(turn, slot):
        shift = (1, 2, -1, -2)[slot]
        side = 0 if shift > 0 else 1
        target = me + shift
        return pltpu.make_async_remote_copy(
            src_ref=ends.at[turn, side], dst_ref=halo.at[turn, slot],
            send_sem=halo_send.at[turn, slot], recv_sem=halo_recv.at[turn, slot],
            device_id=(lax.rem(target + n_dev, n_dev),), device_id_type=pl.DeviceIdType.MESH)

    def sends(slot):
        shift = (1, 2, -1, -2)[slot]
        return (me + shift < n_dev) if shift > 0 else (me + shift >= 0)

    def receives(slot):
        shift = (1, 2, -1, -2)[slot]
        return (me - shift >= 0) if shift > 0 else (me - shift < n_dev)

    def halo_start(turn):
        for slot in range(4):
            @pl.when(sends(slot))
            def _():
                halo_copy(turn, slot).start()

    def halo_wait(turn):
        for slot in range(4):
            @pl.when(receives(slot))
            def _():
                halo_copy(turn, slot).wait_recv()
        for slot in range(4):
            @pl.when(sends(slot))
            def _():
                halo_copy(turn, slot).wait_send()

    halo_start(0)
    halo_wait(0)

    def ghosts(turn, rows):
        a = [halo[turn, s] for s in range(4)]
        left_two = halo[0, 0, 6:7, 0:BLK] > 0.5
        right_two = halo[0, 2, 6:7, BLK:] > 0.5
        l1 = a[0][:, BLK:]
        l0 = jnp.where(left_two, a[0][:, 0:BLK], a[1][:, BLK:])
        r0 = a[2][:, 0:BLK]
        r1 = jnp.where(right_two, a[2][:, BLK:], a[3][:, 0:BLK])
        parts = (l0, l1, r0, r1)
        return [jnp.concatenate([p[rows:rows + 3, :], jnp.zeros((5, BLK), F32)], axis=0) for p in parts]

    first = halo[0, 0]
    left1_live = first[6:7, BLK:] > 0.5
    left0_live = jnp.where(first[6:7, 0:BLK] > 0.5, first[6:7, 0:BLK], halo[0, 1, 6:7, BLK:]) > 0.5
    right0_live = halo[0, 2, 6:7, 0:BLK] > 0.5
    right1_live = jnp.where(halo[0, 2, 6:7, BLK:] > 0.5, halo[0, 2, 6:7, BLK:], halo[0, 3, 6:7, 0:BLK]) > 0.5
    left_two = first[6:7, 0:BLK] > 0.5
    right_two = halo[0, 2, 6:7, BLK:] > 0.5
    gp = ghosts(0, 0)
    gp[0] = jnp.where(left0_live, jnp.where(row8 == 0, gp[0] + jnp.where(left_two, 0.0, -0.5), gp[0]), FAR)
    gp[1] = jnp.where(left1_live, gp[1], FAR)
    gp[2] = jnp.where(right0_live, jnp.where(row8 == 0, gp[2] + countf * 0.5, gp[2]), FAR)
    gp[3] = jnp.where(right1_live, jnp.where(row8 == 0, gp[3] + (countf + jnp.where(right_two, 0.0, 1.0)) * 0.5, gp[3]), FAR)
    gz = ghosts(0, 3)

    wide_block = lax.broadcasted_iota(jnp.int32, (8, width + 2 * BLK), 1) >> 7
    at0 = wide_block == count
    at1 = wide_block == count + 1

    def extended(mid, tail, g):
        whole = jnp.concatenate([mid, tail], axis=1)
        whole = jnp.where(at0, jnp.concatenate([g[2]] * (nb + 2), axis=1), whole)
        whole = jnp.where(at1, jnp.concatenate([g[3]] * (nb + 2), axis=1), whole)
        return whole

    points[:, 0:BLK] = gp[0]
    points[:, BLK:2 * BLK] = gp[1]
    points[:, 2 * BLK:] = extended(points[:, 2 * BLK:2 * BLK + width], jnp.full((8, 2 * BLK), FAR, F32), gp)

    def turn_block(e, carry):
        at = pl.multiple_of(e * BLK, BLK)
        columns[pl.ds(at, BLK), :] = jnp.transpose(points[:, pl.ds(at, BLK)])
        return carry

    lax.fori_loop(0, nb + 4, turn_block, 0)

    def build_wing(b, carry):
        at = pl.multiple_of(b * BLK, BLK)
        here = points[:, pl.ds(pl.multiple_of(at + 2 * BLK, BLK), BLK)]
        build(kmat.at[b], columns, at, [here[c:c + 1, :] for c in range(3)])
        return carry

    lax.fori_loop(0, nb, build_wing, 0)

    def put_vector(turn, g):
        rows = slice(16 * turn, 16 * turn + 16)
        vext[rows, 0:BLK] = split(g[0])
        vext[rows, BLK:2 * BLK] = split(g[1])
        vext[rows, 2 * BLK:] = split(extended(zbuf[...], jnp.zeros((8, 2 * BLK), F32), g))

    def apply(turn):
        rows = slice(16 * turn, 16 * turn + 16)
        step = 4

        def group(q, carry):
            for u in range(step):
                b = q * step + u
                at = pl.multiple_of(b * BLK, BLK)
                o = jnp.dot(vext[rows, pl.ds(at, BAND * BLK)], kmat[b], preferred_element_type=F32)
                ibuf[:, pl.ds(at, BLK)] = o[0:8, 0:BLK] + o[8:16, 0:BLK] + o[0:8, BLK:]
            return carry

        lax.fori_loop(0, nb // step, group, 0)
        ibuf[...] = jnp.where(block_of < count, ibuf[...] + smooth_ref[...] * zbuf[...], 0.0)

    def lanes_sum(v):
        total = v[:, 0:BLK]
        for b in range(1, nb):
            total = total + v[:, b * BLK:(b + 1) * BLK]
        return jnp.sum(total, axis=1, keepdims=True)

    def sums_start(turn):
        norm = lanes_sum(rbuf[...] * zbuf[...])
        prod = lanes_sum(zbuf[...] * ibuf[...])
        spread = jnp.where(lane8 == row8, norm, 0.0) + jnp.where(lane8 == row8 + 8, prod, 0.0)
        sums[turn, me] = jnp.sum(spread, axis=0, keepdims=True)

        def send(k, carry):
            pltpu.make_async_remote_copy(
                src_ref=sums.at[turn, me], dst_ref=sums.at[turn, me],
                send_sem=sum_send.at[turn], recv_sem=sum_recv.at[turn],
                device_id=(lax.rem(me + k, n_dev),), device_id_type=pl.DeviceIdType.MESH).start()
            return carry

        lax.fori_loop(1, n_dev, send, 0)

    def sums_wait(turn):
        others = sums.at[turn, pl.ds(0, n_dev - 1)]
        pltpu.make_async_copy(others, others, sum_recv.at[turn]).wait()
        pltpu.make_async_copy(others, others, sum_send.at[turn]).wait()
        total = jnp.broadcast_to(jnp.sum(sums[turn], axis=0), (8, BLK))
        norm = jnp.sum(jnp.where(lane8 == row8, total, 0.0), axis=1, keepdims=True)
        prod = jnp.sum(jnp.where(lane8 == row8 + 8, total, 0.0), axis=1, keepdims=True)
        return norm, prod

    real = lax.broadcasted_iota(jnp.int32, (8, 1), 0) < 3

    def ratio(a, b):
        return jnp.where(real, a / jnp.where(real, b, 1.0), 0.0)

    ga = None
    norm_now = step_size = None
    gd = gc = None
    for turn in range(ITERS):
        put_vector(turn, gz)
        apply(turn)
        sums_start(turn)
        if turn + 1 < ITERS:
            wbuf[...] = ibuf[...] * inv[...]
            ends[turn + 1, 0, :, 0:BLK] = picked(wbuf, 0, count - 2)
            ends[turn + 1, 0, :, BLK:] = picked(wbuf, 0, count - 1)
            ends[turn + 1, 1, :, :] = wbuf[:, 0:2 * BLK]
            halo_start(turn + 1)
        norm_next, product = sums_wait(turn)
        if turn == 0:
            step_size = ratio(norm_next, product)
            dbuf[...] = zbuf[...]
            abuf[...] = ibuf[...]
            momentum = jnp.zeros((8, 1), F32)
            cbuf[...] = step_size * dbuf[...]
        else:
            momentum = ratio(norm_next, norm_now)
            step_size = ratio(norm_next, product - momentum * ratio(norm_next, step_size))
            dbuf[...] = zbuf[...] + momentum * dbuf[...]
            abuf[...] = ibuf[...] + momentum * abuf[...]
            cbuf[...] = cbuf[...] + step_size * dbuf[...]
        gd = gz if gd is None else [z + momentum * d for z, d in zip(gz, gd)]
        gc = [step_size * d for d in gd] if gc is None else [c + step_size * d for c, d in zip(gc, gd)]
        norm_now = norm_next
        rbuf[...] = rbuf[...] - step_size * abuf[...]
        if turn + 1 < ITERS:
            zbuf[...] = rbuf[...] * inv[...]
            halo_wait(turn + 1)
            gw = ghosts(turn + 1, 0)
            ga = gw if ga is None else [w + momentum * a for w, a in zip(gw, ga)]
            gz = [z - step_size * a for z, a in zip(gz, ga)]
    coef_out[...] = cbuf[0:3, :]
    resid_out[...] = rbuf[0:3, :]
    coef_ext[:, 0:BLK] = gc[0]
    coef_ext[:, BLK:2 * BLK] = gc[1]
    coef_ext[:, 2 * BLK:] = extended(cbuf[...], jnp.zeros((8, 2 * BLK), F32), gc)


def evaluator(nb, fb, live_ref, fluid_ref, points, coef_ext, fluid_out, columns, fpoints, vext, fmat, result):
    count = live_ref[0]
    fpoints[...] = jnp.zeros_like(fpoints)
    fpoints[0:3, :] = fluid_ref[...]
    vext[...] = split(coef_ext[...])

    def turn_block(e, carry):
        at = pl.multiple_of(e * BLK, BLK)
        columns[pl.ds(at, BLK), :] = jnp.transpose(points[:, pl.ds(at, BLK)])
        return carry

    lax.fori_loop(0, nb + 4, turn_block, 0)

    def block(f, slot):
        at = pl.multiple_of(f * BLK, BLK)
        anchor = lax.div(f * count, jnp.int32(fb))
        start = pl.multiple_of(anchor * BLK, BLK)
        here = fpoints[:, pl.ds(at, BLK)]
        row = [here[0:1, :] * 0.5 + anchor.astype(F32) * 0.5, here[1:2, :] * 3.0, here[2:3, :] * 3.0]
        build(fmat.at[slot], columns, start, row)
        o = jnp.dot(vext[:, pl.ds(start, BAND * BLK)], fmat[slot], preferred_element_type=F32)
        result[:, pl.ds(at, BLK)] = o[0:8, 0:BLK] + o[8:16, 0:BLK] + o[0:8, BLK:]

    def pair(q, carry):
        block(2 * q, 0)
        block(2 * q + 1, 1)
        return carry

    lax.fori_loop(0, fb // 2, pair, 0)
    fluid_out[...] = result[0:3, :]


def per_device(n_dev, wing_jitter, live_blocks, smoothing, displacement, fluid_jitter):
    width = wing_jitter.shape[1]
    fwidth = fluid_jitter.shape[1]
    nb = width // BLK
    fb = fwidth // BLK
    vmem = pl.BlockSpec(memory_space=pltpu.VMEM)
    wide = pltpu.VMEM((8, width), F32)
    ext = jax.ShapeDtypeStruct((8, width + 4 * BLK), F32)
    coefs, residual, points, coef_ext = pl.pallas_call(
        functools.partial(solver, n_dev, nb),
        name="solver",
        out_shape=(
            jax.ShapeDtypeStruct((3, width), F32),
            jax.ShapeDtypeStruct((3, width), F32),
            ext, ext,
        ),
        in_specs=[pl.BlockSpec(memory_space=pltpu.SMEM)] + [vmem] * 3,
        out_specs=(vmem,) * 4,
        scratch_shapes=[
            pltpu.VMEM((nb, BAND * BLK, 2 * BLK), BF16),
            pltpu.VMEM((width + 4 * BLK, 8), F32),
            pltpu.VMEM((ITERS, 2, 8, 2 * BLK), F32),
            pltpu.VMEM((ITERS, 4, 8, 2 * BLK), F32),
            pltpu.VMEM((ITERS, n_dev, 1, BLK), F32),
            pltpu.VMEM((16 * ITERS, width + 4 * BLK), BF16),
            wide, wide, wide, wide, wide, wide, wide, wide,
            pltpu.SemaphoreType.DMA((ITERS, 4)),
            pltpu.SemaphoreType.DMA((ITERS, 4)),
            pltpu.SemaphoreType.DMA((ITERS,)),
            pltpu.SemaphoreType.DMA((ITERS,)),
        ],
        compiler_params=pltpu.CompilerParams(
            collective_id=0, has_side_effects=True, vmem_limit_bytes=48 * 1024 * 1024),
    )(live_blocks, wing_jitter, smoothing.reshape(1, width), displacement)
    fluid_values = pl.pallas_call(
        functools.partial(evaluator, nb, fb),
        name="evaluator",
        out_shape=jax.ShapeDtypeStruct((3, fwidth), F32),
        in_specs=[pl.BlockSpec(memory_space=pltpu.SMEM)] + [vmem] * 3,
        out_specs=vmem,
        scratch_shapes=[
            pltpu.VMEM((width + 4 * BLK, 8), F32),
            pltpu.VMEM((8, fwidth), F32),
            pltpu.VMEM((16, width + 4 * BLK), BF16),
            pltpu.VMEM((2, BAND * BLK, 2 * BLK), BF16),
            pltpu.VMEM((8, fwidth), F32),
        ],
        compiler_params=pltpu.CompilerParams(vmem_limit_bytes=16 * 1024 * 1024),
    )(live_blocks, fluid_jitter, points, coef_ext)
    return coefs, residual, fluid_values


def solution(mesh):
    return jax.shard_map(
        functools.partial(per_device, mesh.shape["dom"]),
        mesh=mesh,
        in_specs=(P(None, "dom"), P("dom"), P("dom"), P(None, "dom"), P(None, "dom")),
        out_specs=(P(None, "dom"), P(None, "dom"), P(None, "dom")),
        check_vma=False,
    )
```

```python
import functools

import jax
import jax.numpy as jnp
from jax import lax
from jax.experimental import pallas as pl
from jax.experimental.pallas import tpu as pltpu
from jax.sharding import PartitionSpec as P

BLK = 128
ITERS = 3
BAND = 5
FAR = 64.0
FEATURES = 48
F32 = jnp.float32
BF16 = jnp.bfloat16


def phi_of(spread):
    spread = jnp.maximum(spread, 1e-30)
    scaled = spread * lax.rsqrt(spread)
    remain = jnp.maximum(1.0 - scaled, 0.0)
    square = remain * remain
    return square * square * (5.0 - 4.0 * remain)


def row_ids(width):
    return lax.broadcasted_iota(jnp.int32, (8, width), 0)


def three_terms(v):
    high = v.astype(BF16).astype(F32)
    rest = v - high
    mid = rest.astype(BF16).astype(F32)
    return high, mid, rest - mid


def column_features(p):
    rows = row_ids(BLK)
    norm = jnp.sum(p * p, axis=0, keepdims=True)
    high, mid, low = three_terms(jnp.where(rows == 3, norm, jnp.where(rows == 4, 1.0, p)))
    return jnp.concatenate([high, high, mid, high, low, mid], axis=0)


def row_features(p, shift):
    rows = row_ids(BLK)
    q = jnp.where(rows == 0, p - shift, p)
    norm = jnp.sum(q * q, axis=0, keepdims=True)
    high, mid, low = three_terms(jnp.where(rows == 3, 1.0, jnp.where(rows == 4, norm, -2.0 * q)))
    return jnp.concatenate([high, mid, high, low, high, mid], axis=0).astype(BF16)


def turn_columns(points, columns, blocks):
    def turn_block(q, carry):
        for u in range(2):
            at = pl.multiple_of((2 * q + u) * BLK, BLK)
            features = column_features(points[:, pl.ds(at, BLK)])
            columns[pl.ds(at, BLK), :] = jnp.transpose(features).astype(BF16)
        return carry

    lax.fori_loop(0, blocks // 2, turn_block, 0)


def build(dest, columns, first_col, here):
    for delta in range(BAND):
        at = pl.multiple_of(first_col + delta * BLK, BLK)
        spread = jnp.dot(columns[pl.ds(at, BLK), :], row_features(here, (delta - BAND // 2) * 0.5),
                         preferred_element_type=F32)
        value = phi_of(spread)
        high = value.astype(BF16)
        low = (value - high.astype(F32)).astype(BF16)
        dest[delta * BLK:(delta + 1) * BLK, 0:BLK] = high
        dest[delta * BLK:(delta + 1) * BLK, BLK:] = low


def split(v):
    high = v.astype(BF16).astype(F32)
    return jnp.concatenate([high, v - high], axis=0).astype(BF16)


def solver(n_dev, nb, live_ref, wing_ref, smooth_ref, disp_ref,
           coef_out, resid_out, points, coef_ext,
           kmat, columns, ends, halo, sums, vext, zbuf, rbuf, dbuf, abuf, cbuf, ibuf, wbuf,
           inv, halo_send, halo_recv, sum_send, sum_recv):
    me = lax.axis_index("dom")
    count = live_ref[0]
    width = nb * BLK
    halo[...] = jnp.zeros_like(halo)
    barrier = pltpu.get_barrier_semaphore()

    def greet(k, carry):
        pl.semaphore_signal(barrier, inc=1, device_id=(lax.rem(me + k, n_dev),),
                            device_id_type=pl.DeviceIdType.MESH)
        return carry

    lax.fori_loop(1, n_dev, greet, 0)

    block_of = lax.broadcasted_iota(jnp.int32, (8, width), 1) >> 7
    live = block_of < count
    row_id = lax.broadcasted_iota(jnp.int32, (8, width), 0)
    zbuf[...] = jnp.zeros_like(zbuf)
    zbuf[0:3, :] = wing_ref[...]
    scale = jnp.where(row_id == 0, 0.5, 3.0)
    pts = zbuf[...] * scale - jnp.where(row_id == 0, 0.0, 1.5)
    pts = jnp.where(row_id < 3, jnp.where(live, pts, FAR), 0.0)
    points[:, 2 * BLK:2 * BLK + width] = pts
    smooth = jnp.broadcast_to(smooth_ref[...], (8, width))
    inv[...] = 1.0 / (1.0 + smooth)
    rbuf[...] = jnp.zeros_like(rbuf)
    rbuf[0:3, :] = disp_ref[...]
    rbuf[...] = jnp.where(live, rbuf[...], 0.0)
    zbuf[...] = rbuf[...] * inv[...]

    row8 = lax.broadcasted_iota(jnp.int32, (8, BLK), 0)
    lane8 = lax.broadcasted_iota(jnp.int32, (8, BLK), 1)

    def picked(ref, start, which):
        total = jnp.zeros((8, BLK), F32)
        for b in range(nb):
            total = total + jnp.where(which == b, ref[:, start + b * BLK:start + (b + 1) * BLK], 0.0)
        return total

    two = (count >= 2).astype(F32)

    def pack(p, z, flag):
        low = jnp.concatenate([p[0:3, :], z[0:3, :], jnp.full((2, BLK), 1.0, F32) * flag], axis=0)
        return low

    own = 2 * BLK
    ends[0, 0, :, 0:BLK] = pack(picked(points, own, count - 2), picked(zbuf, 0, count - 2), two)
    ends[0, 0, :, BLK:] = pack(picked(points, own, count - 1), picked(zbuf, 0, count - 1), 1.0)
    ends[0, 1, :, 0:BLK] = pack(points[:, own:own + BLK], zbuf[:, 0:BLK], 1.0)
    ends[0, 1, :, BLK:] = pack(points[:, own + BLK:own + 2 * BLK], zbuf[:, BLK:2 * BLK], two)
    pl.semaphore_wait(barrier, n_dev - 1)

    def halo_copy(turn, slot):
        shift = (1, 2, -1, -2)[slot]
        side = 0 if shift > 0 else 1
        target = me + shift
        return pltpu.make_async_remote_copy(
            src_ref=ends.at[turn, side], dst_ref=halo.at[turn, slot],
            send_sem=halo_send.at[turn, slot], recv_sem=halo_recv.at[turn, slot],
            device_id=(lax.rem(target + n_dev, n_dev),), device_id_type=pl.DeviceIdType.MESH)

    def sends(slot):
        shift = (1, 2, -1, -2)[slot]
        return (me + shift < n_dev) if shift > 0 else (me + shift >= 0)

    def receives(slot):
        shift = (1, 2, -1, -2)[slot]
        return (me - shift >= 0) if shift > 0 else (me - shift < n_dev)

    def halo_start(turn):
        for slot in range(4):
            @pl.when(sends(slot))
            def _():
                halo_copy(turn, slot).start()

    def halo_wait(turn):
        for slot in range(4):
            @pl.when(receives(slot))
            def _():
                halo_copy(turn, slot).wait_recv()
        for slot in range(4):
            @pl.when(sends(slot))
            def _():
                halo_copy(turn, slot).wait_send()

    halo_start(0)
    halo_wait(0)

    def ghosts(turn, rows):
        a = [halo[turn, s] for s in range(4)]
        left_two = halo[0, 0, 6:7, 0:BLK] > 0.5
        right_two = halo[0, 2, 6:7, BLK:] > 0.5
        l1 = a[0][:, BLK:]
        l0 = jnp.where(left_two, a[0][:, 0:BLK], a[1][:, BLK:])
        r0 = a[2][:, 0:BLK]
        r1 = jnp.where(right_two, a[2][:, BLK:], a[3][:, 0:BLK])
        parts = (l0, l1, r0, r1)
        return [jnp.concatenate([p[rows:rows + 3, :], jnp.zeros((5, BLK), F32)], axis=0) for p in parts]

    first = halo[0, 0]
    left1_live = first[6:7, BLK:] > 0.5
    left0_live = jnp.where(first[6:7, 0:BLK] > 0.5, first[6:7, 0:BLK], halo[0, 1, 6:7, BLK:]) > 0.5
    right0_live = halo[0, 2, 6:7, 0:BLK] > 0.5
    right1_live = jnp.where(halo[0, 2, 6:7, BLK:] > 0.5, halo[0, 2, 6:7, BLK:], halo[0, 3, 6:7, 0:BLK]) > 0.5
    gp = ghosts(0, 0)
    away = jnp.where(row8 < 3, FAR, 0.0)
    gp = [jnp.where(seen, g, away) for seen, g in zip((left0_live, left1_live, right0_live, right1_live), gp)]
    gz = ghosts(0, 3)

    wide_block = lax.broadcasted_iota(jnp.int32, (8, width + 2 * BLK), 1) >> 7
    at0 = wide_block == count
    at1 = wide_block == count + 1

    def extended(mid, tail, g):
        whole = jnp.concatenate([mid, tail], axis=1)
        whole = jnp.where(at0, jnp.concatenate([g[2]] * (nb + 2), axis=1), whole)
        whole = jnp.where(at1, jnp.concatenate([g[3]] * (nb + 2), axis=1), whole)
        return whole

    points[:, 0:BLK] = gp[0]
    points[:, BLK:2 * BLK] = gp[1]
    points[:, 2 * BLK:] = extended(points[:, 2 * BLK:2 * BLK + width], jnp.concatenate([away, away], axis=1), gp)

    turn_columns(points, columns, nb + 4)

    def build_wing(q, carry):
        for u in range(2):
            b = 2 * q + u
            at = pl.multiple_of(b * BLK, BLK)
            build(kmat.at[b], columns, at, points[:, pl.ds(pl.multiple_of(at + 2 * BLK, BLK), BLK)])
        return carry

    lax.fori_loop(0, nb // 2, build_wing, 0)

    def put_vector(turn, g):
        rows = slice(16 * turn, 16 * turn + 16)
        vext[rows, 0:BLK] = split(g[0])
        vext[rows, BLK:2 * BLK] = split(g[1])
        vext[rows, 2 * BLK:] = split(extended(zbuf[...], jnp.zeros((8, 2 * BLK), F32), g))

    def apply(turn):
        rows = slice(16 * turn, 16 * turn + 16)
        step = 4

        def group(q, carry):
            for u in range(step):
                b = q * step + u
                at = pl.multiple_of(b * BLK, BLK)
                o = jnp.dot(vext[rows, pl.ds(at, BAND * BLK)], kmat[b], preferred_element_type=F32)
                ibuf[:, pl.ds(at, BLK)] = o[0:8, 0:BLK] + o[8:16, 0:BLK] + o[0:8, BLK:]
            return carry

        lax.fori_loop(0, nb // step, group, 0)
        ibuf[...] = jnp.where(block_of < count, ibuf[...] + smooth_ref[...] * zbuf[...], 0.0)

    def lanes_sum(v):
        total = v[:, 0:BLK]
        for b in range(1, nb):
            total = total + v[:, b * BLK:(b + 1) * BLK]
        return jnp.sum(total, axis=1, keepdims=True)

    def sums_start(turn):
        norm = lanes_sum(rbuf[...] * zbuf[...])
        prod = lanes_sum(zbuf[...] * ibuf[...])
        spread = jnp.where(lane8 == row8, norm, 0.0) + jnp.where(lane8 == row8 + 8, prod, 0.0)
        sums[turn, me] = jnp.sum(spread, axis=0, keepdims=True)

        def send(k, carry):
            pltpu.make_async_remote_copy(
                src_ref=sums.at[turn, me], dst_ref=sums.at[turn, me],
                send_sem=sum_send.at[turn], recv_sem=sum_recv.at[turn],
                device_id=(lax.rem(me + k, n_dev),), device_id_type=pl.DeviceIdType.MESH).start()
            return carry

        lax.fori_loop(1, n_dev, send, 0)

    def sums_wait(turn):
        others = sums.at[turn, pl.ds(0, n_dev - 1)]
        pltpu.make_async_copy(others, others, sum_recv.at[turn]).wait()
        pltpu.make_async_copy(others, others, sum_send.at[turn]).wait()
        total = jnp.broadcast_to(jnp.sum(sums[turn], axis=0), (8, BLK))
        norm = jnp.sum(jnp.where(lane8 == row8, total, 0.0), axis=1, keepdims=True)
        prod = jnp.sum(jnp.where(lane8 == row8 + 8, total, 0.0), axis=1, keepdims=True)
        return norm, prod

    real = lax.broadcasted_iota(jnp.int32, (8, 1), 0) < 3

    def ratio(a, b):
        return jnp.where(real, a / jnp.where(real, b, 1.0), 0.0)

    ga = None
    norm_now = step_size = None
    gd = gc = None
    for turn in range(ITERS):
        put_vector(turn, gz)
        apply(turn)
        sums_start(turn)
        if turn + 1 < ITERS:
            wbuf[...] = ibuf[...] * inv[...]
            ends[turn + 1, 0, :, 0:BLK] = picked(wbuf, 0, count - 2)
            ends[turn + 1, 0, :, BLK:] = picked(wbuf, 0, count - 1)
            ends[turn + 1, 1, :, :] = wbuf[:, 0:2 * BLK]
            halo_start(turn + 1)
        norm_next, product = sums_wait(turn)
        if turn == 0:
            step_size = ratio(norm_next, product)
            dbuf[...] = zbuf[...]
            abuf[...] = ibuf[...]
            momentum = jnp.zeros((8, 1), F32)
            cbuf[...] = step_size * dbuf[...]
        else:
            momentum = ratio(norm_next, norm_now)
            step_size = ratio(norm_next, product - momentum * ratio(norm_next, step_size))
            dbuf[...] = zbuf[...] + momentum * dbuf[...]
            abuf[...] = ibuf[...] + momentum * abuf[...]
            cbuf[...] = cbuf[...] + step_size * dbuf[...]
        gd = gz if gd is None else [z + momentum * d for z, d in zip(gz, gd)]
        gc = [step_size * d for d in gd] if gc is None else [c + step_size * d for c, d in zip(gc, gd)]
        norm_now = norm_next
        rbuf[...] = rbuf[...] - step_size * abuf[...]
        if turn + 1 < ITERS:
            zbuf[...] = rbuf[...] * inv[...]
            halo_wait(turn + 1)
            gw = ghosts(turn + 1, 0)
            ga = gw if ga is None else [w + momentum * a for w, a in zip(gw, ga)]
            gz = [z - step_size * a for z, a in zip(gz, ga)]
    coef_out[...] = cbuf[0:3, :]
    resid_out[...] = rbuf[0:3, :]
    coef_ext[:, 0:BLK] = gc[0]
    coef_ext[:, BLK:2 * BLK] = gc[1]
    coef_ext[:, 2 * BLK:] = extended(cbuf[...], jnp.zeros((8, 2 * BLK), F32), gc)


def evaluator(nb, fb, live_ref, fluid_ref, points, coef_ext, fluid_out, columns, fpoints, vext, fmat, result):
    count = live_ref[0]
    fpoints[...] = jnp.zeros_like(fpoints)
    fpoints[0:3, :] = fluid_ref[...]
    rows = row_ids(fpoints.shape[1])
    fpoints[...] = fpoints[...] * jnp.where(rows == 0, 0.5, 3.0) - jnp.where((rows == 1) | (rows == 2), 1.5, 0.0)
    vext[...] = split(coef_ext[...])

    turn_columns(points, columns, nb + 4)

    def block(f, slot):
        at = pl.multiple_of(f * BLK, BLK)
        anchor = lax.div(f * count, jnp.int32(fb))
        start = pl.multiple_of(anchor * BLK, BLK)
        here = fpoints[:, pl.ds(at, BLK)]
        build(fmat.at[slot], columns, start, here)
        o = jnp.dot(vext[:, pl.ds(start, BAND * BLK)], fmat[slot], preferred_element_type=F32)
        result[:, pl.ds(at, BLK)] = o[0:8, 0:BLK] + o[8:16, 0:BLK] + o[0:8, BLK:]

    def pair(q, carry):
        block(2 * q, 0)
        block(2 * q + 1, 1)
        return carry

    lax.fori_loop(0, fb // 2, pair, 0)
    fluid_out[...] = result[0:3, :]


def per_device(n_dev, wing_jitter, live_blocks, smoothing, displacement, fluid_jitter):
    width = wing_jitter.shape[1]
    fwidth = fluid_jitter.shape[1]
    nb = width // BLK
    fb = fwidth // BLK
    vmem = pl.BlockSpec(memory_space=pltpu.VMEM)
    wide = pltpu.VMEM((8, width), F32)
    ext = jax.ShapeDtypeStruct((8, width + 4 * BLK), F32)
    coefs, residual, points, coef_ext = pl.pallas_call(
        functools.partial(solver, n_dev, nb),
        name="solver",
        out_shape=(
            jax.ShapeDtypeStruct((3, width), F32),
            jax.ShapeDtypeStruct((3, width), F32),
            ext, ext,
        ),
        in_specs=[pl.BlockSpec(memory_space=pltpu.SMEM)] + [vmem] * 3,
        out_specs=(vmem,) * 4,
        scratch_shapes=[
            pltpu.VMEM((nb, BAND * BLK, 2 * BLK), BF16),
            pltpu.VMEM((width + 4 * BLK, FEATURES), BF16),
            pltpu.VMEM((ITERS, 2, 8, 2 * BLK), F32),
            pltpu.VMEM((ITERS, 4, 8, 2 * BLK), F32),
            pltpu.VMEM((ITERS, n_dev, 1, BLK), F32),
            pltpu.VMEM((16 * ITERS, width + 4 * BLK), BF16),
            wide, wide, wide, wide, wide, wide, wide, wide,
            pltpu.SemaphoreType.DMA((ITERS, 4)),
            pltpu.SemaphoreType.DMA((ITERS, 4)),
            pltpu.SemaphoreType.DMA((ITERS,)),
            pltpu.SemaphoreType.DMA((ITERS,)),
        ],
        compiler_params=pltpu.CompilerParams(
            collective_id=0, has_side_effects=True, vmem_limit_bytes=48 * 1024 * 1024),
    )(live_blocks, wing_jitter, smoothing.reshape(1, width), displacement)
    fluid_values = pl.pallas_call(
        functools.partial(evaluator, nb, fb),
        name="evaluator",
        out_shape=jax.ShapeDtypeStruct((3, fwidth), F32),
        in_specs=[pl.BlockSpec(memory_space=pltpu.SMEM)] + [vmem] * 3,
        out_specs=vmem,
        scratch_shapes=[
            pltpu.VMEM((width + 4 * BLK, FEATURES), BF16),
            pltpu.VMEM((8, fwidth), F32),
            pltpu.VMEM((16, width + 4 * BLK), BF16),
            pltpu.VMEM((2, BAND * BLK, 2 * BLK), BF16),
            pltpu.VMEM((8, fwidth), F32),
        ],
        compiler_params=pltpu.CompilerParams(vmem_limit_bytes=16 * 1024 * 1024),
    )(live_blocks, fluid_jitter, points, coef_ext)
    return coefs, residual, fluid_values


def solution(mesh):
    return jax.shard_map(
        functools.partial(per_device, mesh.shape["dom"]),
        mesh=mesh,
        in_specs=(P(None, "dom"), P("dom"), P("dom"), P(None, "dom"), P(None, "dom")),
        out_specs=(P(None, "dom"), P(None, "dom"), P(None, "dom")),
        check_vma=False,
    )
```
